32 devices in a mesh: gx: 8 (over y, x, core), gy: 4 (over z).
Axes of the slice: x: 2, y: 2, z: 4, core: 2. Of those that a mesh axis runs over, the one named last changes fastest.
Arguments:
- coefficients: float32 [2, 2048, 512], P(None, 'gx', 'gy'), may hold values from -0.125 to 0.125
- spacing: float32 [31], replicated, may hold values from 0.6 to 1.5
Outputs:
- zcoord: float32 [32, 4096, 512], P(None, 'gx', 'gy')
- slopes: float32 [2, 32, 4096, 512], P(None, None, 'gx', 'gy')
- jacobian: float32 [32, 4096, 512], P(None, 'gx', 'gy')
- quality: float32 [32, 4096, 512], P(None, 'gx', 'gy')
The draws below stay inside these ranges and needn't reach their ends.
All inputs are finite; a program needn't handle non-finite values.
Results may differ from the reference program's by a relative error of at most 0.0003.
Values sent between devices are 32-bit elements; how exact they have to be, the bound alone decides.
A program may use at most 128 MiB of HBM per device.

```python
import math
import jax
import jax.numpy as jnp
from jax import lax

NX = 4096
MODES = 2048
NY = 512
GAPS = 31


def shard_levels(own_key, shape, shards, least, high):
    factor_of, own = 1.0, jax.random.fold_in(own_key, 6)
    for axis_at, shards_of in shards:
        steps = jnp.exp(jax.random.uniform(jax.random.fold_in(own, axis_at), (shards_of,), jnp.float32, least / len(shards), high / len(shards)))
        factor_of = factor_of * jnp.repeat(steps, shape[axis_at] // shards_of).reshape([-1 if axis == axis_at else 1 for axis in range(len(shape))])
    return factor_of


def bell_draw(stream_key, dims, scale, reach, split=(), held_as=jnp.bfloat16):
    drawn = scale * jax.random.normal(stream_key, dims, jnp.float32)
    if split:
        drawn = drawn * shard_levels(stream_key, dims, split, -0.22, 0.18)
    return jnp.clip(drawn, -reach, reach).astype(held_as)


def setup_inputs(seed: int = 0) -> dict:
    streams_of = jax.random.split(jax.random.key(seed), 3)
    coefficients = bell_draw(streams_of[0], (2, MODES, NY), MODES ** -0.5, 0.125, ((1, 8), (2, 4)), jnp.float32)
    spacing = jnp.clip(jnp.exp(jax.random.uniform(streams_of[1], (GAPS,), jnp.float32, math.log(0.6), math.log(1.5))), 0.6, 1.5)
    return {"coefficients": coefficients, "spacing": spacing}


BOUNDARY = ((-24.0 / 17.0, 59.0 / 34.0, -4.0 / 17.0, -3.0 / 34.0, 0.0, 0.0), (-0.5, 0.0, 0.5, 0.0, 0.0, 0.0), (4.0 / 43.0, -59.0 / 86.0, 0.0, 59.0 / 86.0, -4.0 / 43.0, 0.0), (3.0 / 98.0, 0.0, -59.0 / 98.0, 0.0, 32.0 / 49.0, -4.0 / 49.0))
TOPO_SCALE = 0.1


def vertical(field):
    levels = field.shape[0]
    top_rows = []
    bottom_rows = []
    for row_id in range(4):
        upper = None
        lower = None
        for level_id, factor in enumerate(BOUNDARY[row_id]):
            if factor != 0.0:
                term_up = factor * field[level_id]
                term_down = -factor * field[levels - 1 - level_id]
                upper = term_up if upper is None else upper + term_up
                lower = term_down if lower is None else lower + term_down
        top_rows.append(upper)
        bottom_rows.append(lower)
    inner = (8.0 * (field[5:levels - 3] - field[3:levels - 5]) - (field[6:levels - 2] - field[2:levels - 6])) / 12.0
    return jnp.concatenate([jnp.stack(top_rows), inner, jnp.stack(bottom_rows[::-1])], axis=0)


def stretching(spacing):
    summed = jnp.sum(spacing)
    return jnp.concatenate([jnp.zeros((1,), spacing.dtype), jnp.cumsum(spacing)]) / summed


def column_depth(surface, stretch):
    levels = stretch.shape[0]
    return (levels - 1.0) * (surface[None] + (1.0 - surface[None]) * stretch[:, None, None])


def across(field, axis_id):
    plus_one = jnp.roll(field, -1, axis_id)
    minus_one = jnp.roll(field, 1, axis_id)
    plus_two = jnp.roll(field, -2, axis_id)
    minus_two = jnp.roll(field, 2, axis_id)
    return (8.0 * (plus_one - minus_one) - (plus_two - minus_two)) / 12.0


def reference(coefficients, spacing):
    mode_ids = jnp.arange(MODES, dtype=jnp.int32)
    x_cells = jnp.arange(NX, dtype=jnp.int32)
    phase = ((mode_ids[:, None] * x_cells[None, :]) % NX).astype(jnp.float32) * (2.0 * math.pi / NX)
    cosine = jnp.cos(phase)
    sine = jnp.sin(phase)
    surface_raw = jnp.dot(cosine.T, coefficients[0], precision=lax.Precision.HIGHEST, preferred_element_type=jnp.float32)
    surface_raw = surface_raw + jnp.dot(sine.T, coefficients[1], precision=lax.Precision.HIGHEST, preferred_element_type=jnp.float32)
    surface = TOPO_SCALE * jnp.tanh(surface_raw * 0.25)
    stretch = stretching(spacing)
    zcoord = column_depth(surface, stretch)
    slopes = jnp.stack([across(zcoord, 1), across(zcoord, 2)])
    jacobian = vertical(zcoord)
    lowest = jnp.min(jacobian)
    quality = jacobian / lowest
    return zcoord, slopes, jacobian, quality
```

```python
import functools
import math

import jax
import jax.numpy as jnp
import numpy as np
from jax import lax
from jax.experimental import pallas as pl
from jax.experimental.pallas import tpu as pltpu
from jax.sharding import PartitionSpec as P

NX = 4096


BOUNDARY = (
    (-24.0 / 17.0, 59.0 / 34.0, -4.0 / 17.0, -3.0 / 34.0, 0.0, 0.0),
    (-0.5, 0.0, 0.5, 0.0, 0.0, 0.0),
    (4.0 / 43.0, -59.0 / 86.0, 0.0, 59.0 / 86.0, -4.0 / 43.0, 0.0),
    (3.0 / 98.0, 0.0, -59.0 / 98.0, 0.0, 32.0 / 49.0, -4.0 / 49.0),
)
TOPO_SCALE = 0.1


def extended(cells, sides, width):
    for axis, dim in sides:
        count = lax.axis_size(axis)
        head = lax.slice_in_dim(cells, 0, width, axis=dim)
        tail = lax.slice_in_dim(cells, cells.shape[dim] - width, cells.shape[dim], axis=dim)
        cells = jnp.concatenate(
            [
                lax.ppermute(tail, axis, [(i, (i + 1) % count) for i in range(count)]),
                cells,
                lax.ppermute(head, axis, [((i + 1) % count, i) for i in range(count)]),
            ],
            axis=dim,
        )
    return cells


def vertical(field):
    levels = field.shape[0]
    top_rows = []
    bottom_rows = []
    for row_id in range(4):
        upper = None
        lower = None
        for level_id, factor in enumerate(BOUNDARY[row_id]):
            if factor != 0.0:
                term_up = factor * field[level_id]
                term_down = -factor * field[levels - 1 - level_id]
                upper = term_up if upper is None else upper + term_up
                lower = term_down if lower is None else lower + term_down
        top_rows.append(upper)
        bottom_rows.append(lower)
    inner = (
        8.0 * (field[5 : levels - 3] - field[3 : levels - 5])
        - (field[6 : levels - 2] - field[2 : levels - 6])
    ) / 12.0
    return jnp.concatenate([jnp.stack(top_rows), inner, jnp.stack(bottom_rows[::-1])], axis=0)


def stretching(spacing):
    summed = jnp.sum(spacing)
    return jnp.concatenate([jnp.zeros((1,), spacing.dtype), jnp.cumsum(spacing)]) / summed


def column_depth(surface, stretch):
    levels = stretch.shape[0]
    return (levels - 1.0) * (surface[None] + (1.0 - surface[None]) * stretch[:, None, None])


def basis(count, x_cells):
    mode_ids = jnp.arange(count, dtype=jnp.int32)
    phase = (mode_ids[:, None] * x_cells[None, :] % NX).astype(jnp.float32) * (2.0 * math.pi / NX)
    return (jnp.cos(phase), jnp.sin(phase))


def project(cosine, sine, portion):
    first = jnp.dot(
        cosine.T, portion[0], precision=lax.Precision.HIGHEST, preferred_element_type=jnp.float32
    )
    return first + jnp.dot(
        sine.T, portion[1], precision=lax.Precision.HIGHEST, preferred_element_type=jnp.float32
    )


LANES = 128
RADIX = 16
TILE = 8
MESH = pl.DeviceIdType.MESH


def level_weights(gaps):
    levels = gaps + 1
    summed = np.tril(np.ones((levels, gaps)), -1)
    deriv = np.zeros((levels, levels))
    for row in range(levels):
        if row < 4:
            deriv[row, :6] = BOUNDARY[row]
        elif row >= levels - 4:
            deriv[row, ::-1][:6] = -np.array(BOUNDARY[levels - 1 - row])
        else:
            deriv[row, row - 2 : row + 3] = np.array([1.0, -8.0, 0.0, 8.0, -1.0]) / 12.0
    return np.stack([summed, deriv @ summed]).astype(np.float32)


def transform_tables(modes, groups):
    part = NX // RADIX
    own = part // groups
    block = own + TILE
    rows = []
    for dest in range(groups):
        first = dest * own
        rows += list(range(first, first + own)) + [first - 1, first + own] + [first] * (TILE - 2)
    angle = 2.0 * np.pi / part * ((np.array(rows)[:, None] * np.arange(part)[None]) % part)
    full = np.concatenate([np.cos(angle), np.sin(angle)], axis=1).astype(np.float32)
    turn = 2.0 * np.pi / NX * (np.arange(RADIX)[:, None] * np.arange(part)[None])
    twiddle = np.concatenate([np.cos(turn), np.sin(turn)], axis=1).astype(np.float32)
    return full, twiddle, block


def rotate(value, angle):
    re, im = value
    cos, sin = math.cos(angle), math.sin(angle)
    if abs(sin) < 1e-12:
        return (re, im) if cos > 0 else (-re, -im)
    if abs(cos) < 1e-12:
        return (im, -re) if sin > 0 else (-im, re)
    if abs(abs(cos) - abs(sin)) < 1e-12:
        unit = math.sqrt(0.5)
        a, b = math.copysign(1.0, cos), math.copysign(1.0, sin)
        one = re * unit if a > 0 else re * -unit
        two = im * unit if a > 0 else im * -unit
        if a == b:
            return one + two, two - one
        return one - two, two + one
    return re * cos + im * sin, im * cos - re * sin


def fourier(values):
    count = len(values)
    if count == 1:
        return values
    even, odd = fourier(values[0::2]), fourier(values[1::2])
    out = [None] * count
    for i in range(count // 2):
        re, im = rotate(odd[i], 2.0 * math.pi * i / count)
        out[i] = (even[i][0] + re, even[i][1] + im)
        out[i + count // 2] = (even[i][0] - re, even[i][1] - im)
    return out


def split(value):
    high = value.astype(jnp.bfloat16)
    return high, (value - high.astype(jnp.float32)).astype(jnp.bfloat16)


def regroup(values, lane, width):
    values = list(values)
    step = len(values) // 2
    while step:
        upper = (lane // width) & step != 0
        shift = step * width
        for i in range(len(values)):
            if not i & step:
                low, high = values[i], values[i + step]
                values[i] = jnp.where(upper, pltpu.roll(high, shift, 1), low)
                values[i + step] = jnp.where(upper, high, pltpu.roll(low, LANES - shift, 1))
        step //= 2
    return values


def surface_kernel(
    groups, columns, coef, spacing, weights, basis_high_hbm, basis_low_hbm, twiddle,
    s_out, dx_out, dy_out, table,
    basis_high, basis_low, turned, gathered, high, low, product, landed, above, below,
    extended_s, outer, best, bests,
    const_sem, send_one, recv_one, send_two, recv_two, send_side, recv_side, send_max, recv_max,
):
    gx, gy = lax.axis_index("gx"), lax.axis_index("gy")
    loads = [
        pltpu.make_async_copy(basis_high_hbm, basis_high, const_sem.at[0]),
        pltpu.make_async_copy(basis_low_hbm, basis_low, const_sem.at[1]),
    ]
    for load in loads:
        load.start()
    barrier = pltpu.get_barrier_semaphore()
    for d in range(1, groups):
        pl.semaphore_signal(
            barrier, inc=1, device_id=(lax.rem(gx + d, groups), gy), device_id_type=MESH
        )
    for d in range(1, columns):
        pl.semaphore_signal(
            barrier, inc=1, device_id=(gx, lax.rem(gy + d, columns)), device_id_type=MESH
        )

    part = coef.shape[1]
    ys = coef.shape[2] // groups
    turned[:, :part] = coef[0].T
    turned[:, part:] = coef[1].T
    pl.semaphore_wait(barrier, groups + columns - 2)

    first = []
    for d in range(1, groups):
        target = lax.rem(gx + d, groups)
        copy = pltpu.make_async_remote_copy(
            src_ref=turned.at[pl.ds(pl.multiple_of(target * ys, TILE), ys)],
            dst_ref=gathered.at[gx],
            send_sem=send_one.at[d],
            recv_sem=recv_one.at[d],
            device_id=(target, gy),
            device_id_type=MESH,
        )
        copy.start()
        first.append(copy)
    gathered[gx] = turned[pl.ds(pl.multiple_of(gx * ys, TILE), ys), :]

    thick = spacing[...]
    total = jnp.sum(thick, axis=1, keepdims=True)
    scale = spacing.shape[1] * 1.0
    levels = spacing.shape[1] + 1
    stretch = jnp.sum(weights[0] * thick, axis=1, keepdims=True) / total
    slope = jnp.sum(weights[1] * thick, axis=1, keepdims=True) / total
    least = jnp.min(slope, axis=0, keepdims=True)
    table[0] = jnp.broadcast_to(scale * stretch, (levels, LANES))
    table[1] = jnp.broadcast_to(scale * (1.0 - stretch), (levels, LANES))
    table[2] = jnp.broadcast_to(scale * slope, (levels, LANES))

    for copy in first:
        copy.wait()

    half = NX // RADIX
    parts = half // part
    values = []
    for i in range(RADIX // 2):
        re = [gathered[i * parts + p, :, :part] for p in range(parts)]
        im = [gathered[i * parts + p, :, part:] for p in range(parts)]
        values.append(
            (re[0], im[0]) if parts == 1 else (jnp.concatenate(re, 1), jnp.concatenate(im, 1))
        )
    even = fourier(values)
    odd = fourier([rotate(v, 2.0 * math.pi * i / RADIX) for i, v in enumerate(values)])
    for r in range(RADIX):
        re, im = (even if r % 2 == 0 else odd)[r // 2]
        if r:
            cos, sin = twiddle[r : r + 1, :half], twiddle[r : r + 1, half:]
            re, im = re * cos + im * sin, im * cos - re * sin
        rows = slice(r * ys, (r + 1) * ys)
        high[rows, :half], low[rows, :half] = split(re)
        high[rows, half:], low[rows, half:] = split(im)

    for load in loads:
        load.wait()
    dot = functools.partial(
        lax.dot_general,
        dimension_numbers=(((1,), (1,)), ((), ())),
        preferred_element_type=jnp.float32,
    )
    raw = dot(basis_high[...], high[...])
    raw = raw + dot(basis_high[...], low[...])
    raw = raw + dot(basis_low[...], high[...])
    product[...] = raw
    block = landed.shape[1]
    own = block - TILE
    top = jnp.max(raw, axis=0, keepdims=True)
    for dest in range(groups):
        product[dest * block + own + 2 : dest * block + own + 3, :] = top

    second = []
    for d in range(1, groups):
        target = lax.rem(gx + d, groups)
        copy = pltpu.make_async_remote_copy(
            src_ref=product.at[pl.ds(pl.multiple_of(target * block, TILE), block)],
            dst_ref=landed.at[gx],
            send_sem=send_two.at[d],
            recv_sem=recv_two.at[d],
            device_id=(target, gy),
            device_id_type=MESH,
        )
        copy.start()
        second.append(copy)
    landed[gx] = product[pl.ds(pl.multiple_of(gx * block, TILE), block), :]
    for copy in second:
        copy.wait()

    side = []
    for i, (source, dest, d) in enumerate(((0, above, columns - 1), (groups - 1, below, 1))):
        copy = pltpu.make_async_remote_copy(
            src_ref=landed.at[source],
            dst_ref=dest,
            send_sem=send_side.at[i],
            recv_sem=recv_side.at[i],
            device_id=(gx, lax.rem(gy + d, columns)),
            device_id_type=MESH,
        )
        copy.start()
        side.append(copy)
    top = landed[0, own + 2 : own + 3, :]
    for j in range(1, groups):
        top = jnp.maximum(top, landed[j, own + 2 : own + 3, :])
    best[...] = jnp.broadcast_to(jnp.max(top, axis=1, keepdims=True), (TILE, LANES))
    maxima = []
    for d in range(1, columns):
        copy = pltpu.make_async_remote_copy(
            src_ref=best,
            dst_ref=bests.at[d],
            send_sem=send_max.at[d],
            recv_sem=recv_max.at[d],
            device_id=(gx, lax.rem(gy + d, columns)),
            device_id_type=MESH,
        )
        copy.start()
        maxima.append(copy)

    count = own * RADIX
    lane = lax.broadcasted_iota(jnp.int32, (block, LANES), 1)
    fold = LANES // ys
    for part_id in range(RADIX // fold):
        lanes = slice(part_id * LANES, (part_id + 1) * LANES)
        pieces = regroup([landed[j, :, lanes] for j in range(groups)], lane, ys)
        for i, piece in enumerate(pieces):
            r = part_id * fold + i
            piece = TOPO_SCALE * jnp.tanh(piece * 0.25)
            extended_s[pl.ds(TILE + r, own, stride=RADIX), :] = piece[:own]
            if r >= RADIX - 2:
                at = TILE - RADIX + r
                extended_s[at : at + 1, :] = piece[own : own + 1]
            if r < 2:
                at = TILE + count + r
                extended_s[at : at + 1, :] = piece[own + 1 : own + 2]
    s_out[...] = extended_s[TILE : TILE + count, :]
    dx_out[...] = (
        8.0 * (extended_s[TILE + 1 : TILE + 1 + count, :] - extended_s[TILE - 1 : TILE - 1 + count, :])
        - (extended_s[TILE + 2 : TILE + 2 + count, :] - extended_s[TILE - 2 : TILE - 2 + count, :])
    ) * (1.0 / 12.0)

    for copy in side:
        copy.wait()
    lane = lax.broadcasted_iota(jnp.int32, (own, LANES), 1)
    for r in range(RADIX):
        lanes = slice(r // fold * LANES, (r // fold + 1) * LANES)
        at = r % fold
        right, left = above[:own, lanes], below[:own, lanes]
        if at:
            right = pltpu.roll(right, LANES - at * ys, 1)
        if at != fold - 1:
            left = pltpu.roll(left, (fold - 1 - at) * ys, 1)
        piece = jnp.where(lane < LANES // 2, right, left)
        outer[pl.ds(r, own, stride=RADIX), :] = TOPO_SCALE * jnp.tanh(piece * 0.25)
    inner, edge = s_out[...], outer[...]
    lane = lax.broadcasted_iota(jnp.int32, (count, LANES), 1)

    def moved(by):
        taken = lane < by if by > 0 else lane >= LANES + by
        return pltpu.roll(jnp.where(taken, edge, inner), (LANES - by) % LANES, 1)

    dy_out[...] = (8.0 * (moved(1) - moved(-1)) - (moved(2) - moved(-2))) * (1.0 / 12.0)

    for copy in maxima:
        copy.wait()
    peak = best[0:1, :]
    for d in range(1, columns):
        peak = jnp.maximum(peak, bests[d, 0:1, :])
    peak = TOPO_SCALE * jnp.tanh(peak * 0.25)
    table[3] = jnp.broadcast_to(slope, (levels, LANES)) / ((1.0 - peak) * least)


def surface_by_kernel(coefficients, spacing, groups, columns):
    _, modes, ys = coefficients.shape
    full, twiddle, block = transform_tables(modes * groups, groups)
    high = full.astype(jnp.bfloat16)
    low = (full - high.astype(np.float32)).astype(jnp.bfloat16)
    weights = level_weights(spacing.shape[0])
    levels = spacing.shape[0] + 1
    count = NX // groups
    part = NX // RADIX
    width = RADIX * (ys // groups)
    vmem = pl.BlockSpec(memory_space=pltpu.VMEM)
    hbm = pl.BlockSpec(memory_space=pl.ANY)
    plane = jax.ShapeDtypeStruct((count, ys), jnp.float32)
    dma = pltpu.SemaphoreType.DMA
    return pl.pallas_call(
        functools.partial(surface_kernel, groups, columns),
        out_shape=(plane, plane, plane, jax.ShapeDtypeStruct((4, levels, LANES), jnp.float32)),
        in_specs=[vmem, vmem, vmem, hbm, hbm, vmem],
        out_specs=(vmem,) * 4,
        scratch_shapes=[
            pltpu.VMEM(full.shape, jnp.bfloat16),
            pltpu.VMEM(full.shape, jnp.bfloat16),
            pltpu.VMEM((ys, 2 * modes), jnp.float32),
            pltpu.VMEM((groups, ys // groups, 2 * modes), jnp.float32),
            pltpu.VMEM((width, 2 * part), jnp.bfloat16),
            pltpu.VMEM((width, 2 * part), jnp.bfloat16),
            pltpu.VMEM((groups * block, width), jnp.float32),
            pltpu.VMEM((groups, block, width), jnp.float32),
            pltpu.VMEM((block, width), jnp.float32),
            pltpu.VMEM((block, width), jnp.float32),
            pltpu.VMEM((count + 2 * TILE, ys), jnp.float32),
            pltpu.VMEM((count, ys), jnp.float32),
            pltpu.VMEM((TILE, LANES), jnp.float32),
            pltpu.VMEM((columns, TILE, LANES), jnp.float32),
            dma((2,)),
            dma((groups,)),
            dma((groups,)),
            dma((groups,)),
            dma((groups,)),
            dma((2,)),
            dma((2,)),
            dma((columns,)),
            dma((columns,)),
        ],
        compiler_params=pltpu.CompilerParams(collective_id=0, has_side_effects=True),
    )(coefficients, spacing[None], jnp.asarray(weights), jnp.asarray(high), jnp.asarray(low), jnp.asarray(twiddle))


def surface_by_gather(coefficients, spacing, groups):
    x_count = NX // groups
    x_first = lax.axis_index("gx") * x_count
    x_cells = x_first + jnp.arange(x_count, dtype=jnp.int32)
    portion = lax.all_gather(coefficients, "gx", axis=1, tiled=True)
    cosine, sine = basis(portion.shape[1], x_cells)
    surface = TOPO_SCALE * jnp.tanh(project(cosine, sine, portion) * 0.25)
    stretch = stretching(spacing)
    scale = stretch.shape[0] - 1.0
    slope = vertical(stretch)
    peak = lax.pmax(jnp.max(surface), ("gx", "gy"))
    wide = extended(surface, (("gx", 0), ("gy", 1)), 2)
    dx = (8.0 * (wide[3:-1] - wide[1:-3]) - (wide[4:] - wide[:-4]))[:, 2:-2] / 12.0
    dy = (8.0 * (wide[:, 3:-1] - wide[:, 1:-3]) - (wide[:, 4:] - wide[:, :-4]))[2:-2] / 12.0
    rows = [scale * stretch, scale * (1.0 - stretch), scale * slope]
    rows.append(slope / ((1.0 - peak) * jnp.min(slope)))
    table = jnp.broadcast_to(jnp.stack(rows)[:, :, None], (4, stretch.shape[0], LANES))
    return surface, dx, dy, table


def levels_kernel(depth, s_ref, dx_ref, dy_ref, table, z_ref, slopes_ref, jac_ref, quality_ref):
    first = pl.program_id(0) * depth

    def row(which, level):
        return table[which, pl.ds(first + level, 1), :]

    for level in range(depth):
        s, gain = s_ref[...], row(1, level)
        z_ref[level] = row(0, level) + gain * s
        slopes_ref[0, level] = gain * dx_ref[...]
        slopes_ref[1, level] = gain * dy_ref[...]
        rest = 1.0 - s
        jac_ref[level] = row(2, level) * rest
        quality_ref[level] = row(3, level) * rest


def all_levels(s, dx, dy, table):
    levels = table.shape[1]
    rows, columns = s.shape
    depth = 2
    plane = pl.BlockSpec((rows, columns), lambda i: (0, 0))
    field = pl.BlockSpec((depth, rows, columns), lambda i: (i, 0, 0))
    shape = jax.ShapeDtypeStruct((levels, rows, columns), jnp.float32)
    return pl.pallas_call(
        functools.partial(levels_kernel, depth),
        grid=(levels // depth,),
        in_specs=[plane, plane, plane, pl.BlockSpec(table.shape, lambda i: (0, 0, 0))],
        out_specs=(
            field,
            pl.BlockSpec((2, depth, rows, columns), lambda i: (0, i, 0, 0)),
            field,
            field,
        ),
        out_shape=(
            shape,
            jax.ShapeDtypeStruct((2, levels, rows, columns), jnp.float32),
            shape,
            shape,
        ),
    )(s, dx, dy, table)


def shards(coefficients, spacing):
    groups, columns = lax.axis_size("gx"), lax.axis_size("gy")
    _, modes, ys = coefficients.shape
    fits = (
        ys == LANES
        and modes % LANES == 0
        and modes * groups * 2 == NX
        and ys % (groups * RADIX) == 0
        and groups * (ys // groups) == LANES
        and (NX // RADIX) % (groups * TILE) == 0
        and columns > 1
    )
    if fits:
        parts = surface_by_kernel(coefficients, spacing, groups, columns)
    else:
        parts = surface_by_gather(coefficients, spacing, groups)
    return all_levels(*parts)


def solution(mesh):
    return jax.shard_map(
        shards,
        mesh=mesh,
        in_specs=(P(None, "gx", "gy"), P()),
        out_specs=(
            P(None, "gx", "gy"),
            P(None, None, "gx", "gy"),
            P(None, "gx", "gy"),
            P(None, "gx", "gy"),
        ),
        check_vma=False,
    )
```

```python
import functools
import math

import jax
import jax.numpy as jnp
import numpy as np
from jax import lax
from jax.experimental import pallas as pl
from jax.experimental.pallas import tpu as pltpu
from jax.sharding import PartitionSpec as P

NX = 4096


BOUNDARY = (
    (-24.0 / 17.0, 59.0 / 34.0, -4.0 / 17.0, -3.0 / 34.0, 0.0, 0.0),
    (-0.5, 0.0, 0.5, 0.0, 0.0, 0.0),
    (4.0 / 43.0, -59.0 / 86.0, 0.0, 59.0 / 86.0, -4.0 / 43.0, 0.0),
    (3.0 / 98.0, 0.0, -59.0 / 98.0, 0.0, 32.0 / 49.0, -4.0 / 49.0),
)
TOPO_SCALE = 0.1


def extended(cells, sides, width):
    for axis, dim in sides:
        count = lax.axis_size(axis)
        head = lax.slice_in_dim(cells, 0, width, axis=dim)
        tail = lax.slice_in_dim(cells, cells.shape[dim] - width, cells.shape[dim], axis=dim)
        cells = jnp.concatenate(
            [
                lax.ppermute(tail, axis, [(i, (i + 1) % count) for i in range(count)]),
                cells,
                lax.ppermute(head, axis, [((i + 1) % count, i) for i in range(count)]),
            ],
            axis=dim,
        )
    return cells


def vertical(field):
    levels = field.shape[0]
    top_rows = []
    bottom_rows = []
    for row_id in range(4):
        upper = None
        lower = None
        for level_id, factor in enumerate(BOUNDARY[row_id]):
            if factor != 0.0:
                term_up = factor * field[level_id]
                term_down = -factor * field[levels - 1 - level_id]
                upper = term_up if upper is None else upper + term_up
                lower = term_down if lower is None else lower + term_down
        top_rows.append(upper)
        bottom_rows.append(lower)
    inner = (
        8.0 * (field[5 : levels - 3] - field[3 : levels - 5])
        - (field[6 : levels - 2] - field[2 : levels - 6])
    ) / 12.0
    return jnp.concatenate([jnp.stack(top_rows), inner, jnp.stack(bottom_rows[::-1])], axis=0)


def stretching(spacing):
    summed = jnp.sum(spacing)
    return jnp.concatenate([jnp.zeros((1,), spacing.dtype), jnp.cumsum(spacing)]) / summed


def column_depth(surface, stretch):
    levels = stretch.shape[0]
    return (levels - 1.0) * (surface[None] + (1.0 - surface[None]) * stretch[:, None, None])


def basis(count, x_cells):
    mode_ids = jnp.arange(count, dtype=jnp.int32)
    phase = (mode_ids[:, None] * x_cells[None, :] % NX).astype(jnp.float32) * (2.0 * math.pi / NX)
    return (jnp.cos(phase), jnp.sin(phase))


def project(cosine, sine, portion):
    first = jnp.dot(
        cosine.T, portion[0], precision=lax.Precision.HIGHEST, preferred_element_type=jnp.float32
    )
    return first + jnp.dot(
        sine.T, portion[1], precision=lax.Precision.HIGHEST, preferred_element_type=jnp.float32
    )


LANES = 128
RADIX = 16
TILE = 8
MESH = pl.DeviceIdType.MESH


def level_weights(gaps):
    levels = gaps + 1
    summed = np.tril(np.ones((levels, gaps)), -1)
    deriv = np.zeros((levels, levels))
    for row in range(levels):
        if row < 4:
            deriv[row, :6] = BOUNDARY[row]
        elif row >= levels - 4:
            deriv[row, ::-1][:6] = -np.array(BOUNDARY[levels - 1 - row])
        else:
            deriv[row, row - 2 : row + 3] = np.array([1.0, -8.0, 0.0, 8.0, -1.0]) / 12.0
    return np.stack([summed, deriv @ summed]).astype(np.float32)


def transform_tables(modes, groups):
    part = NX // RADIX
    own = part // groups
    block = own + TILE
    rows = []
    for dest in range(groups):
        first = dest * own
        rows += list(range(first, first + own)) + [first - 1, first + own] + [first] * (TILE - 2)
    angle = 2.0 * np.pi / part * ((np.array(rows)[:, None] * np.arange(part)[None]) % part)
    full = np.concatenate([np.cos(angle), np.sin(angle)], axis=1).astype(np.float32)
    turn = 2.0 * np.pi / NX * (np.arange(RADIX)[:, None] * np.arange(part)[None])
    twiddle = np.concatenate([np.cos(turn), np.sin(turn)], axis=1).astype(np.float32)
    return full, twiddle, block


def rotate(value, angle):
    re, im = value
    cos, sin = math.cos(angle), math.sin(angle)
    if abs(sin) < 1e-12:
        return (re, im) if cos > 0 else (-re, -im)
    if abs(cos) < 1e-12:
        return (im, -re) if sin > 0 else (-im, re)
    if abs(abs(cos) - abs(sin)) < 1e-12:
        unit = math.sqrt(0.5)
        a, b = math.copysign(1.0, cos), math.copysign(1.0, sin)
        one = re * unit if a > 0 else re * -unit
        two = im * unit if a > 0 else im * -unit
        if a == b:
            return one + two, two - one
        return one - two, two + one
    return re * cos + im * sin, im * cos - re * sin


def fourier(values):
    count = len(values)
    if count == 1:
        return values
    even, odd = fourier(values[0::2]), fourier(values[1::2])
    out = [None] * count
    for i in range(count // 2):
        re, im = rotate(odd[i], 2.0 * math.pi * i / count)
        out[i] = (even[i][0] + re, even[i][1] + im)
        out[i + count // 2] = (even[i][0] - re, even[i][1] - im)
    return out


def split(value):
    high = value.astype(jnp.bfloat16)
    return high, (value - high.astype(jnp.float32)).astype(jnp.bfloat16)


def regroup(values, lane, width):
    values = list(values)
    step = len(values) // 2
    while step:
        upper = (lane // width) & step != 0
        shift = step * width
        for i in range(len(values)):
            if not i & step:
                low, high = values[i], values[i + step]
                values[i] = jnp.where(upper, pltpu.roll(high, shift, 1), low)
                values[i + step] = jnp.where(upper, high, pltpu.roll(low, LANES - shift, 1))
        step //= 2
    return values


def surface_kernel(
    groups, columns, coef, spacing, weights, basis_high_hbm, basis_low_hbm, twiddle,
    s_out, dx_out, dy_out, table,
    basis_high, basis_low, turned, gathered, high, low, product, landed, above, below,
    extended_s, outer, best, bests, edges, edge_product,
    const_sem, send_one, recv_one, send_two, recv_two, send_side, recv_side, send_max, recv_max,
):
    gx, gy = lax.axis_index("gx"), lax.axis_index("gy")

    def moved_by(d):
        return lax.rem(gx + d // columns, groups), lax.rem(gy + d % columns, columns)

    loads = [
        pltpu.make_async_copy(basis_high_hbm, basis_high, const_sem.at[0]),
        pltpu.make_async_copy(basis_low_hbm, basis_low, const_sem.at[1]),
    ]
    for load in loads:
        load.start()
    barrier = pltpu.get_barrier_semaphore()
    for d in range(1, groups * columns):
        pl.semaphore_signal(barrier, inc=1, device_id=moved_by(d), device_id_type=MESH)

    part = coef.shape[1]
    ys = coef.shape[2] // groups
    turned[:, :part] = coef[0].T
    turned[:, part:] = coef[1].T
    pl.semaphore_wait(barrier, groups * columns - 1)

    first = []
    for d in range(1, groups):
        target = lax.rem(gx + d, groups)
        copy = pltpu.make_async_remote_copy(
            src_ref=turned.at[pl.ds(pl.multiple_of(target * ys, TILE), ys)],
            dst_ref=gathered.at[gx],
            send_sem=send_one.at[d],
            recv_sem=recv_one.at[d],
            device_id=(target, gy),
            device_id_type=MESH,
        )
        copy.start()
        first.append(copy)
    gathered[gx] = turned[pl.ds(pl.multiple_of(gx * ys, TILE), ys), :]

    thick = spacing[...]
    total = jnp.sum(thick, axis=1, keepdims=True)
    scale = spacing.shape[1] * 1.0
    levels = spacing.shape[1] + 1
    stretch = jnp.sum(weights[0] * thick, axis=1, keepdims=True) / total
    slope = jnp.sum(weights[1] * thick, axis=1, keepdims=True) / total
    least = jnp.min(slope, axis=0, keepdims=True)
    table[0] = jnp.broadcast_to(scale * stretch, (levels, LANES))
    table[1] = jnp.broadcast_to(scale * (1.0 - stretch), (levels, LANES))
    table[2] = jnp.broadcast_to(scale * slope, (levels, LANES))

    for copy in first:
        copy.wait()

    half = NX // RADIX
    parts = half // part
    values = []
    for i in range(RADIX // 2):
        re = [gathered[i * parts + p, :, :part] for p in range(parts)]
        im = [gathered[i * parts + p, :, part:] for p in range(parts)]
        values.append(
            (re[0], im[0]) if parts == 1 else (jnp.concatenate(re, 1), jnp.concatenate(im, 1))
        )
    even = fourier(values)
    odd = fourier([rotate(v, 2.0 * math.pi * i / RADIX) for i, v in enumerate(values)])
    for r in range(RADIX):
        re, im = (even if r % 2 == 0 else odd)[r // 2]
        if r:
            cos, sin = twiddle[r : r + 1, :half], twiddle[r : r + 1, half:]
            re, im = re * cos + im * sin, im * cos - re * sin
        rows = slice(r * ys, (r + 1) * ys)
        high[rows, :half], low[rows, :half] = split(re)
        high[rows, half:], low[rows, half:] = split(im)
        rows = slice(r * TILE, (r + 1) * TILE)
        edges[rows, :half] = jnp.where(gx == 0, re[:TILE], re[ys - TILE :])
        edges[rows, half:] = jnp.where(gx == 0, im[:TILE], im[ys - TILE :])

    for load in loads:
        load.wait()
    dot = functools.partial(
        lax.dot_general,
        dimension_numbers=(((1,), (1,)), ((), ())),
        preferred_element_type=jnp.float32,
    )
    raw = dot(basis_high[...], high[...])
    raw = raw + dot(basis_high[...], low[...])
    raw = raw + dot(basis_low[...], high[...])
    best[...] = jnp.broadcast_to(jnp.max(raw, keepdims=True), (TILE, LANES))
    maxima = []
    for d in range(1, groups * columns):
        copy = pltpu.make_async_remote_copy(
            src_ref=best,
            dst_ref=bests.at[d],
            send_sem=send_max.at[d],
            recv_sem=recv_max.at[d],
            device_id=moved_by(d),
            device_id_type=MESH,
        )
        copy.start()
        maxima.append(copy)
    block = basis_high.shape[0] // groups
    own = block - TILE
    sublane = lax.broadcasted_iota(jnp.int32, (TILE, LANES), 0)
    for dest in range(groups):
        rows = raw[dest * block : (dest + 1) * block]
        product[dest, :own] = rows[:own, :LANES]
        product[dest, own : 2 * own] = rows[:own, LANES:]
        product[dest, 2 * own :] = jnp.where(sublane == 0, rows[own:, LANES:], rows[own:, :LANES])

    second = []
    for d in range(1, groups):
        target = lax.rem(gx + d, groups)
        copy = pltpu.make_async_remote_copy(
            src_ref=product.at[target],
            dst_ref=landed.at[gx],
            send_sem=send_two.at[d],
            recv_sem=recv_two.at[d],
            device_id=(target, gy),
            device_id_type=MESH,
        )
        copy.start()
        second.append(copy)
    landed[gx] = product[gx]

    edge_high, edge_low = split(edges[...])
    raw = dot(basis_high[...], edge_high)
    raw = raw + dot(basis_high[...], edge_low)
    raw = raw + dot(basis_low[...], edge_high)
    for dest in range(groups):
        edge_product[dest] = raw[dest * block : dest * block + own]

    def side_copy(which, dest):
        return pltpu.make_async_remote_copy(
            src_ref=edge_product.at[dest],
            dst_ref=(above, below)[which],
            send_sem=send_side.at[dest],
            recv_sem=recv_side.at[which],
            device_id=(dest, lax.rem(gy + (columns - 1, 1)[which], columns)),
            device_id_type=MESH,
        )

    for which, sender in enumerate((0, groups - 1)):

        @pl.when(gx == sender)
        def _():
            for dest in range(groups):
                side_copy(which, dest).start()

    for copy in second:
        copy.wait()

    count = own * RADIX
    lane = lax.broadcasted_iota(jnp.int32, (own, LANES), 1)
    for part_id in range(RADIX // groups):
        rows = slice(part_id * own, (part_id + 1) * own)
        pieces = regroup([landed[j, rows, :] for j in range(groups)], lane, ys)
        for i, piece in enumerate(pieces):
            r = part_id * groups + i
            extended_s[pl.ds(TILE + r, own, stride=RADIX), :] = TOPO_SCALE * jnp.tanh(piece * 0.25)
    lane = lax.broadcasted_iota(jnp.int32, (TILE, LANES), 1)
    pieces = regroup([landed[j, 2 * own :, :] for j in range(groups)], lane, ys)
    for i in range(2):
        before = TOPO_SCALE * jnp.tanh(pieces[groups - 2 + i] * 0.25)
        after = TOPO_SCALE * jnp.tanh(pieces[i] * 0.25)
        extended_s[TILE - 2 + i : TILE - 1 + i, :] = before[0:1]
        extended_s[TILE + count + i : TILE + count + i + 1, :] = after[1:2]
    s_out[...] = extended_s[TILE : TILE + count, :]
    dx_out[...] = (
        8.0 * (extended_s[TILE + 1 : TILE + 1 + count, :] - extended_s[TILE - 1 : TILE - 1 + count, :])
        - (extended_s[TILE + 2 : TILE + 2 + count, :] - extended_s[TILE - 2 : TILE - 2 + count, :])
    ) * (1.0 / 12.0)

    for which, sender in enumerate((0, groups - 1)):
        side_copy(which, 0).wait_recv()

        @pl.when(gx == sender)
        def _():
            for dest in range(groups):
                side_copy(which, dest).wait_send()

    lane = lax.broadcasted_iota(jnp.int32, (own, LANES), 1)
    right_all = TOPO_SCALE * jnp.tanh(above[...] * 0.25)
    left_all = TOPO_SCALE * jnp.tanh(below[...] * 0.25)
    for r in range(RADIX):
        right = pltpu.roll(right_all, LANES - r * TILE, 1) if r else right_all
        left = pltpu.roll(left_all, LANES - TILE - r * TILE, 1) if r != RADIX - 1 else left_all
        outer[pl.ds(r, own, stride=RADIX), :] = jnp.where(lane < LANES // 2, right, left)
    inner, edge = s_out[...], outer[...]
    lane = lax.broadcasted_iota(jnp.int32, (count, LANES), 1)

    def moved(by):
        taken = lane < by if by > 0 else lane >= LANES + by
        return pltpu.roll(jnp.where(taken, edge, inner), (LANES - by) % LANES, 1)

    dy_out[...] = (8.0 * (moved(1) - moved(-1)) - (moved(2) - moved(-2))) * (1.0 / 12.0)

    for copy in maxima:
        copy.wait()
    peak = best[0:1, :]
    for d in range(1, groups * columns):
        peak = jnp.maximum(peak, bests[d, 0:1, :])
    peak = TOPO_SCALE * jnp.tanh(peak * 0.25)
    table[3] = jnp.broadcast_to(slope, (levels, LANES)) / ((1.0 - peak) * least)


def surface_by_kernel(coefficients, spacing, groups, columns):
    _, modes, ys = coefficients.shape
    full, twiddle, block = transform_tables(modes * groups, groups)
    high = full.astype(jnp.bfloat16)
    low = (full - high.astype(np.float32)).astype(jnp.bfloat16)
    weights = level_weights(spacing.shape[0])
    levels = spacing.shape[0] + 1
    count = NX // groups
    part = NX // RADIX
    width = RADIX * (ys // groups)
    own = block - TILE
    vmem = pl.BlockSpec(memory_space=pltpu.VMEM)
    hbm = pl.BlockSpec(memory_space=pl.ANY)
    plane = jax.ShapeDtypeStruct((count, ys), jnp.float32)
    dma = pltpu.SemaphoreType.DMA
    return pl.pallas_call(
        functools.partial(surface_kernel, groups, columns),
        out_shape=(plane, plane, plane, jax.ShapeDtypeStruct((4, levels, LANES), jnp.float32)),
        in_specs=[vmem, vmem, vmem, hbm, hbm, vmem],
        out_specs=(vmem,) * 4,
        scratch_shapes=[
            pltpu.VMEM(full.shape, jnp.bfloat16),
            pltpu.VMEM(full.shape, jnp.bfloat16),
            pltpu.VMEM((ys, 2 * modes), jnp.float32),
            pltpu.VMEM((groups, ys // groups, 2 * modes), jnp.float32),
            pltpu.VMEM((width, 2 * part), jnp.bfloat16),
            pltpu.VMEM((width, 2 * part), jnp.bfloat16),
            pltpu.VMEM((groups, 2 * own + TILE, LANES), jnp.float32),
            pltpu.VMEM((groups, 2 * own + TILE, LANES), jnp.float32),
            pltpu.VMEM((own, LANES), jnp.float32),
            pltpu.VMEM((own, LANES), jnp.float32),
            pltpu.VMEM((count + 2 * TILE, ys), jnp.float32),
            pltpu.VMEM((count, ys), jnp.float32),
            pltpu.VMEM((TILE, LANES), jnp.float32),
            pltpu.VMEM((groups * columns, TILE, LANES), jnp.float32),
            pltpu.VMEM((RADIX * TILE, 2 * part), jnp.float32),
            pltpu.VMEM((groups, own, LANES), jnp.float32),
            dma((2,)),
            dma((groups,)),
            dma((groups,)),
            dma((groups,)),
            dma((groups,)),
            dma((groups,)),
            dma((2,)),
            dma((groups * columns,)),
            dma((groups * columns,)),
        ],
        compiler_params=pltpu.CompilerParams(collective_id=0, has_side_effects=True),
    )(coefficients, spacing[None], jnp.asarray(weights), jnp.asarray(high), jnp.asarray(low), jnp.asarray(twiddle))


def surface_by_gather(coefficients, spacing, groups):
    x_count = NX // groups
    x_first = lax.axis_index("gx") * x_count
    x_cells = x_first + jnp.arange(x_count, dtype=jnp.int32)
    portion = lax.all_gather(coefficients, "gx", axis=1, tiled=True)
    cosine, sine = basis(portion.shape[1], x_cells)
    surface = TOPO_SCALE * jnp.tanh(project(cosine, sine, portion) * 0.25)
    stretch = stretching(spacing)
    scale = stretch.shape[0] - 1.0
    slope = vertical(stretch)
    peak = lax.pmax(jnp.max(surface), ("gx", "gy"))
    wide = extended(surface, (("gx", 0), ("gy", 1)), 2)
    dx = (8.0 * (wide[3:-1] - wide[1:-3]) - (wide[4:] - wide[:-4]))[:, 2:-2] / 12.0
    dy = (8.0 * (wide[:, 3:-1] - wide[:, 1:-3]) - (wide[:, 4:] - wide[:, :-4]))[2:-2] / 12.0
    rows = [scale * stretch, scale * (1.0 - stretch), scale * slope]
    rows.append(slope / ((1.0 - peak) * jnp.min(slope)))
    table = jnp.broadcast_to(jnp.stack(rows)[:, :, None], (4, stretch.shape[0], LANES))
    return surface, dx, dy, table


def levels_kernel(depth, s_ref, dx_ref, dy_ref, table, z_ref, slopes_ref, jac_ref, quality_ref):
    first = pl.program_id(0) * depth

    def row(which, level):
        return table[which, pl.ds(first + level, 1), :]

    for level in range(depth):
        s, gain = s_ref[...], row(1, level)
        z_ref[level] = row(0, level) + gain * s
        slopes_ref[0, level] = gain * dx_ref[...]
        slopes_ref[1, level] = gain * dy_ref[...]
        rest = 1.0 - s
        jac_ref[level] = row(2, level) * rest
        quality_ref[level] = row(3, level) * rest


def all_levels(s, dx, dy, table):
    levels = table.shape[1]
    rows, columns = s.shape
    depth = 2
    plane = pl.BlockSpec((rows, columns), lambda i: (0, 0))
    field = pl.BlockSpec((depth, rows, columns), lambda i: (i, 0, 0))
    shape = jax.ShapeDtypeStruct((levels, rows, columns), jnp.float32)
    return pl.pallas_call(
        functools.partial(levels_kernel, depth),
        grid=(levels // depth,),
        in_specs=[plane, plane, plane, pl.BlockSpec(table.shape, lambda i: (0, 0, 0))],
        out_specs=(
            field,
            pl.BlockSpec((2, depth, rows, columns), lambda i: (0, i, 0, 0)),
            field,
            field,
        ),
        out_shape=(
            shape,
            jax.ShapeDtypeStruct((2, levels, rows, columns), jnp.float32),
            shape,
            shape,
        ),
    )(s, dx, dy, table)


def shards(coefficients, spacing):
    groups, columns = lax.axis_size("gx"), lax.axis_size("gy")
    _, modes, ys = coefficients.shape
    fits = (
        ys == LANES
        and modes % LANES == 0
        and modes * groups * 2 == NX
        and ys % (groups * RADIX) == 0
        and ys == groups * RADIX
        and groups * TILE * 2 == RADIX * TILE
        and (NX // RADIX) % (groups * TILE) == 0
        and columns > 1
    )
    if fits:
        parts = surface_by_kernel(coefficients, spacing, groups, columns)
    else:
        parts = surface_by_gather(coefficients, spacing, groups)
    return all_levels(*parts)


def solution(mesh):
    return jax.shard_map(
        shards,
        mesh=mesh,
        in_specs=(P(None, "gx", "gy"), P()),
        out_specs=(
            P(None, "gx", "gy"),
            P(None, None, "gx", "gy"),
            P(None, "gx", "gy"),
            P(None, "gx", "gy"),
        ),
        check_vma=False,
    )
```
